128 devices in a mesh: grp: 4 (over z_lo, core), dp: 32 (over z_hi, y, x).
Axes of the slice: x: 4, y: 4, z: 4 (z_hi: 2, z_lo: 2; z = z_hi * 2 + z_lo), core: 2. Of those that a mesh axis runs over, the one named last changes fastest.
Arguments:
- activations: bfloat16 [262144, 1280], P(('grp', 'dp')), may hold values from -6 to 6
- cotangent: bfloat16 [262144, 1280], P(('grp', 'dp')), may hold values from -0.01171875 to 0.01171875
- carried_error: float32 [128, 1280, 1280], P(('grp', 'dp')), may hold values from -6 to 6
- owner_error: float32 [1280, 1280], P(('grp', 'dp')), may hold values from -6 to 6
Outputs:
- update: float32 [1280, 1280], replicated
The draws below stay inside these ranges and needn't reach their ends.
All inputs are finite; a program needn't handle non-finite values.
Results may differ from the reference program's by a relative error of at most 0.012.
Values may be sent and summed in bfloat16 or wider, within the bound.
A program may use at most 128 MiB of HBM per device.

```python
import jax
import jax.numpy as jnp
from jax import lax

D = 1280
BLOCK = 128
TOK_DEV = 2048
TOKENS = 262144
N_GRP = 4
N_DP = 32
DEVICES = 128


def strengthened(entries, stream_key, source, target, shards_of, factor):
    owner, partner = [(jnp.arange(entries.shape[position]) // (entries.shape[position] // shards_of)).reshape([-1 if axis == position else 1 for axis in range(entries.ndim)]) for position in (source, target)]
    chosen = jax.random.permutation(stream_key, shards_of)[partner]
    strong = (owner == chosen) | (owner == (partner + shards_of // 2) % shards_of)
    return jnp.where(strong, factor * entries, entries)


def shard_levels(own_key, shape, split, low, top_value):
    def one(axis_at, blocks):
        heights = jax.random.uniform(jax.random.fold_in(jax.random.fold_in(own_key, 6), axis_at), (blocks,), jnp.float32, low / len(split), top_value / len(split))
        return jnp.repeat(jnp.exp(heights), shape[axis_at] // blocks).reshape((-1,) + (1,) * (len(shape) - axis_at - 1))

    factor_of = one(*split[0])
    for cut in split[1:]:
        factor_of = factor_of * one(*cut)
    return factor_of


def bell_draw(stream_key, dims, spread, bound, cuts=(), kind=jnp.bfloat16):
    level = shard_levels(stream_key, dims, cuts, -0.22, 0.18) if cuts else 1.0
    values = jax.random.normal(stream_key, dims, jnp.float32) * spread * level
    return jnp.minimum(jnp.maximum(values, -bound), bound).astype(kind)


def gaussian_with(stream_key, dims, deviation, bound, shards, heavy, kind=jnp.bfloat16):
    values = deviation * jax.random.normal(stream_key, dims, jnp.float32)
    if shards:
        values = values * shard_levels(stream_key, dims, shards, -0.22, 0.18)
    return jnp.clip(strengthened(values, jax.random.fold_in(stream_key, 3), *heavy), -bound, bound).astype(kind)


def setup_inputs(seed: int = 0) -> dict:
    key_of = jax.random.split(jax.random.key(seed), 5)
    return {
        "activations": bell_draw(key_of[0], (TOKENS, D), 1.0, 6.0, ((0, 128),)),
        "cotangent": bell_draw(key_of[1], (TOKENS, D), (TOK_DEV * N_GRP * N_DP) ** -0.5, 0.01171875, ((0, 128),)),
        "carried_error": gaussian_with(key_of[2], (DEVICES, D, D), 0.1, 6.0, ((0, 128),), (0, 1, 128, 5.5), jnp.float32),
        "owner_error": bell_draw(key_of[3], (D, D), 0.5, 6.0, ((0, 128),), jnp.float32),
    }


def quantize(values):
    blocks = values.reshape(values.shape[:-1] + (values.shape[-1] // BLOCK, BLOCK))
    largest = jnp.max(jnp.abs(blocks), axis=-1)
    scales = ((largest + 1e-6) / 127.0).astype(jnp.bfloat16)
    levels = (blocks / scales.astype(jnp.float32)[..., None]).astype(jnp.bfloat16)
    return levels.reshape(values.shape), scales


def dequantize(levels, scales):
    blocks = levels.reshape(levels.shape[:-1] + (levels.shape[-1] // BLOCK, BLOCK)).astype(jnp.float32)
    return (blocks * scales.astype(jnp.float32)[..., None]).reshape(levels.shape)


def reference(activations, cotangent, carried_error, owner_error):
    inputs_dev = activations.reshape(DEVICES, TOK_DEV, D)
    grads_dev = cotangent.reshape(DEVICES, TOK_DEV, D)

    def add_device(summed, pieces):
        inputs_one, grads_one, error_one = pieces
        gradient = lax.dot_general(inputs_one.astype(jnp.float32), grads_one.astype(jnp.float32), (((0,), (0,)), ((), ())), preferred_element_type=jnp.float32)
        levels, scales = quantize(gradient + error_one)
        return summed + dequantize(levels, scales), None

    summed, unused = lax.scan(add_device, jnp.zeros((D, D), jnp.float32), (inputs_dev, grads_dev, carried_error))
    summed = summed + owner_error
    owner_level, owner_scale = quantize(summed)
    return dequantize(owner_level, owner_scale)
```

```python
import jax
import jax.numpy as jnp
from jax import lax
from jax.sharding import PartitionSpec as P

D = 1280
BLOCK = 128


def quantize(values):
    blocks = values.reshape(values.shape[:-1] + (values.shape[-1] // BLOCK, BLOCK))
    largest = jnp.max(jnp.abs(blocks), axis=-1)
    scales = ((largest + 1e-06) / 127.0).astype(jnp.bfloat16)
    levels = (blocks / scales.astype(jnp.float32)[..., None]).astype(jnp.bfloat16)
    return (levels.reshape(values.shape), scales)


def dequantize(levels, scales):
    blocks = levels.reshape(levels.shape[:-1] + (levels.shape[-1] // BLOCK, BLOCK)).astype(
        jnp.float32
    )
    return (blocks * scales.astype(jnp.float32)[..., None]).reshape(levels.shape)


def on_device(activations, cotangent, carried_error, owner_error):
    gradient = lax.dot_general(
        activations, cotangent, (((0,), (0,)), ((), ())), preferred_element_type=jnp.float32
    )
    own = dequantize(*quantize(gradient + carried_error[0]))
    rows = owner_error.shape[0]
    start = rows * (lax.axis_index("grp") * lax.axis_size("dp") + lax.axis_index("dp"))
    mine = lax.dynamic_slice_in_dim(own, start, rows, 0) + owner_error
    own = lax.dynamic_update_slice_in_dim(own, mine, start, 0)
    summed = lax.psum(own.astype(jnp.bfloat16), ("grp", "dp")).astype(jnp.float32)
    return dequantize(*quantize(summed))


def solution(mesh):
    return jax.shard_map(
        on_device,
        mesh=mesh,
        in_specs=(
            P(("grp", "dp"), None),
            P(("grp", "dp"), None),
            P(("grp", "dp"), None, None),
            P(("grp", "dp"), None),
        ),
        out_specs=P(),
        check_vma=False,
    )
```

```python
import jax
import jax.numpy as jnp
from jax import lax
from jax.experimental import pallas as pl
from jax.experimental.pallas import tpu as pltpu
from jax.sharding import PartitionSpec as P

D = 1280
BLOCK = 128
TOK = 2048
MESH = pl.DeviceIdType.MESH
B = 5
ROWS = D // B
TILES = ROWS // 8
HALF = 5
KS = (3, 3, 2)
OFFS = (0, 12, 24)
KOFF = (0, 3, 6)
ORDER = (("z", "y", "x"), ("y", "x", "z"), ("x", "z", "y"))
GROUPS = ((0, 2), (2, 3))


def quantized(x):
    largest = jnp.max(jnp.abs(x), axis=-1, keepdims=True)
    scale = ((largest + 1e-06) / 127.0).astype(jnp.bfloat16).astype(jnp.float32)
    level = (x * (1.0 / scale)).astype(jnp.bfloat16).astype(jnp.float32)
    return level * scale


def places():
    g, d = lax.axis_index("grp"), lax.axis_index("dp")
    return {
        "core": lax.rem(g, 2),
        "z": 2 * (d // 16) + g // 2,
        "y": lax.rem(d // 4, 4),
        "x": lax.rem(d, 4),
    }


def device_at(place):
    z = place["z"]
    return (2 * lax.rem(z, 2) + place["core"], 16 * (z // 2) + 4 * place["y"] + place["x"])


def along(place, axis, step):
    return {**place, axis: lax.rem(place[axis] + step, 4)}


def reduce_kernel(
    a_hbm, c_hbm, e_hbm, oe_ref, g_ref,
    a_v, c_v, e_v, at_v, pad_v, q, rx0, s, r1, t, r2, v, r3,
    a_sem, c_sem, e_sem, d2d_recv, p1_recv, p2_recv, p3_recv, g3_recv, g2_recv, g1_recv, gd_recv, sent,
):
    me = places()
    core = me["core"]
    partner = {**me, "core": 1 - core}
    peers = [partner] + [along(me, axis, step) for axis in "xyz" for step in (1, 2, 3)]
    barrier = pltpu.get_barrier_semaphore()
    for peer in peers:
        pl.semaphore_signal(barrier, inc=1, device_id=device_at(peer), device_id_type=MESH)

    def load_a(b):
        return pltpu.make_async_copy(a_hbm.at[:, pl.ds(b * ROWS, ROWS)], a_v.at[b], a_sem.at[b])

    def load_e(b):
        return pltpu.make_async_copy(e_hbm.at[0, pl.ds(b * ROWS, ROWS), :], e_v.at[b], e_sem.at[b])

    load_c = pltpu.make_async_copy(c_hbm, c_v, c_sem)
    load_a(0).start()
    load_c.start()
    for b in range(B):
        if b:
            load_a(b).start()
        load_e(b).start()

    def push(src, dst, peer, send, recv):
        pltpu.make_async_remote_copy(
            src_ref=src, dst_ref=dst, send_sem=send, recv_sem=recv,
            device_id=device_at(peer), device_id_type=MESH,
        ).start()

    def landed(ref, sem):
        pltpu.make_async_copy(ref, ref, sem).wait()

    index = lax.axis_index("grp") * 32 + lax.axis_index("dp")
    first_tile = (10 * index) // 8
    shift = 10 * index - 8 * first_tile
    row = lax.broadcasted_iota(jnp.int32, (16, D), 0)
    padded = jnp.zeros((16, D), jnp.float32)
    for r in range(10):
        padded = jnp.where(row == shift + r, oe_ref[r : r + 1, :], padded)
    pad_v[...] = padded

    pl.semaphore_wait(barrier, len(peers))
    load_c.wait()

    def multiply(b):
        load_a(b).wait()
        at_v[...] = a_v[b].T
        load_e(b).wait()
        for n in range(5):
            x = jnp.dot(at_v[...], c_v[:, n * 256 : (n + 1) * 256], preferred_element_type=jnp.float32)
            x = x + e_v[b, :, n * 256 : (n + 1) * 256]
            for u in range(2):
                h, j = divmod(2 * n + u, HALF)
                own = quantized(x[:, u * 128 : (u + 1) * 128])
                q[b, h, :, j] = own.astype(jnp.bfloat16).reshape(TILES, 8, 128)
        for w in range(2):
            tile = first_tile + w

            @pl.when(tile // TILES == b)
            def _():
                i = lax.rem(tile, TILES)
                for h in range(2):
                    for j in range(HALF):
                        col = (h * HALF + j) * 128
                        was = q[b, h, i, j].astype(jnp.float32)
                        q[b, h, i, j] = (was + pad_v[w * 8 : w * 8 + 8, col : col + 128]).astype(jnp.bfloat16)

        push(q.at[b, 1 - core], rx0.at[b], partner, sent.at[0], d2d_recv.at[b])

    def chip_sum(b):
        landed(rx0.at[b], d2d_recv.at[b])
        s[b] = (q[b, core].astype(jnp.float32) + rx0[b].astype(jnp.float32)).astype(jnp.bfloat16)
        for c in range(3):
            for step in (2, 1, 3):
                peer = along(me, ORDER[c][0], step)
                at = OFFS[c] + peer[ORDER[c][0]] * KS[c]
                push(
                    s.at[b, pl.ds(at, KS[c])], r1.at[b, step - 1, pl.ds(KOFF[c], KS[c])],
                    peer, sent.at[1], p1_recv.at[b],
                )

    def first_sum(b):
        landed(r1.at[b], p1_recv.at[b])
        for c in range(3):
            total = s[b, pl.ds(OFFS[c] + me[ORDER[c][0]] * KS[c], KS[c])].astype(jnp.float32)
            for step in range(3):
                total = total + r1[b, step, KOFF[c] : KOFF[c] + KS[c]].astype(jnp.float32)
            t[b, c, 0 : 5 * KS[c]] = total.astype(jnp.bfloat16).reshape(5 * KS[c], 8, 128)

    def second_send(i):
        b, nb = GROUPS[i]
        for c in range(3):
            for step in (2, 1, 3):
                peer = along(me, ORDER[c][1], step)
                push(
                    t.at[pl.ds(b, nb), c, pl.ds(4 * peer[ORDER[c][1]], 4)], r2.at[pl.ds(b, nb), step - 1, c],
                    peer, sent.at[2], p2_recv.at[i],
                )

    def second_sum(i):
        b, nb = GROUPS[i]
        landed(r2.at[pl.ds(b, nb)], p2_recv.at[i])
        for c in range(3):
            total = t[b : b + nb, c, pl.ds(4 * me[ORDER[c][1]], 4)].astype(jnp.float32)
            for step in range(3):
                total = total + r2[b : b + nb, step, c].astype(jnp.float32)
            v[b : b + nb, c] = total.astype(jnp.bfloat16)
        for c in range(3):
            for step in (2, 1, 3):
                peer = along(me, ORDER[c][2], step)
                push(
                    v.at[pl.ds(b, nb), c, peer[ORDER[c][2]]], r3.at[pl.ds(b, nb), step - 1, c],
                    peer, sent.at[3], p3_recv.at[i],
                )

    def spread(i, level, recv):
        b, nb = GROUPS[i]
        for c in range(3):
            p1, p2, p3 = (me[axis] for axis in ORDER[c])
            for step in (2, 1, 3):
                if level == 2:
                    ref = g_ref.at[core, pl.ds(b, nb), c, p1, 4 * p2 + p3]
                elif level == 1:
                    ref = g_ref.at[core, pl.ds(b, nb), c, p1, pl.ds(4 * p2, 4)]
                else:
                    ref = g_ref.at[core, pl.ds(b, nb), c, p1, pl.ds(0, 5 * KS[c])]
                push(ref, ref, along(me, ORDER[c][level], step), sent.at[4 + level], recv)

    def own_update(i):
        b, nb = GROUPS[i]
        landed(r3.at[pl.ds(b, nb)], p3_recv.at[i])
        for c in range(3):
            p1, p2, p3 = (me[axis] for axis in ORDER[c])
            total = v[b : b + nb, c, p3].astype(jnp.float32)
            for step in range(3):
                total = total + r3[b : b + nb, step, c].astype(jnp.float32)
            g_ref[core, b : b + nb, c, p1, 4 * p2 + p3] = quantized(total).astype(jnp.bfloat16)
        spread(i, 2, g3_recv.at[i])

    def gathered(i, level, sem):
        b, nb = GROUPS[i]
        if level == 0:
            landed(r1.at[pl.ds(b, nb)], sem.at[i])
        elif level == 1:
            landed(r2.at[pl.ds(b, nb), :, :, :], sem.at[i])
        else:
            landed(r3.at[pl.ds(b, nb)], sem.at[i])

    def to_partner(i):
        b, nb = GROUPS[i]
        gathered(i, 0, g1_recv)
        push(g_ref.at[core, pl.ds(b, nb)], g_ref.at[core, pl.ds(b, nb)], partner, sent.at[7], gd_recv.at[i])

    def step(b, carry):
        multiply(b)

        @pl.when(b >= 1)
        def _():
            chip_sum(b - 1)

        @pl.when(b >= 3)
        def _():
            first_sum(b - 3)

        return carry

    lax.fori_loop(0, B, step, 0)
    second_send(0)
    chip_sum(B - 1)
    for b in range(2, B):
        first_sum(b)
    second_sum(0)
    second_send(1)
    own_update(0)
    second_sum(1)
    gathered(0, 2, g3_recv)
    spread(0, 1, g2_recv.at[0])
    own_update(1)
    gathered(0, 1, g2_recv)
    spread(0, 0, g1_recv.at[0])
    gathered(1, 2, g3_recv)
    spread(1, 1, g2_recv.at[1])
    gathered(1, 1, g2_recv)
    spread(1, 0, g1_recv.at[1])
    to_partner(0)
    to_partner(1)
    for i, (b, nb) in enumerate(GROUPS):
        landed(g_ref.at[1 - core, pl.ds(b, nb)], gd_recv.at[i])
    landed(rx0, sent.at[0])
    landed(r1, sent.at[1])
    landed(r2, sent.at[2])
    landed(r3, sent.at[3])
    landed(r1, sent.at[4])
    landed(r2, sent.at[5])
    landed(r3, sent.at[6])
    landed(g_ref.at[0], sent.at[7])


def expand_kernel(g_ref, out_ref):
    for h in range(2):
        for c in range(3):
            for a in range(4):
                for k in range(KS[c]):
                    row = 8 * (OFFS[c] + a * KS[c] + k)
                    for j in range(HALF):
                        col = (h * HALF + j) * 128
                        out_ref[row : row + 8, col : col + 128] = g_ref[h, 0, c, a, 5 * k + j].astype(jnp.float32)


def on_device(activations, cotangent, carried_error, owner_error):
    any_spec = pl.BlockSpec(memory_space=pl.ANY)
    bf16, f32, dma = jnp.bfloat16, jnp.float32, pltpu.SemaphoreType.DMA
    shape = (2, B, 3, 4, 16, 8, 128)
    ng = len(GROUPS)
    gathered = pl.pallas_call(
        reduce_kernel,
        out_shape=jax.ShapeDtypeStruct(shape, bf16),
        in_specs=[any_spec, any_spec, any_spec, pl.BlockSpec(memory_space=pltpu.VMEM)],
        out_specs=pl.BlockSpec(memory_space=pltpu.VMEM),
        scratch_shapes=[
            pltpu.VMEM((B, TOK, ROWS), bf16),
            pltpu.VMEM((TOK, D), bf16),
            pltpu.VMEM((B, ROWS, D), f32),
            pltpu.VMEM((ROWS, TOK), bf16),
            pltpu.VMEM((16, D), f32),
            pltpu.VMEM((B, 2, TILES, HALF, 8, 128), bf16),
            pltpu.VMEM((B, TILES, HALF, 8, 128), bf16),
            pltpu.VMEM((B, TILES, HALF, 8, 128), bf16),
            pltpu.VMEM((B, 3, 8, HALF, 8, 128), bf16),
            pltpu.VMEM((B, 3, 16, 8, 128), bf16),
            pltpu.VMEM((B, 3, 3, 4, 8, 128), bf16),
            pltpu.VMEM((B, 3, 4, 8, 128), bf16),
            pltpu.VMEM((B, 3, 3, 8, 128), bf16),
            dma((B,)), dma, dma((B,)), dma((B,)), dma((B,)),
            dma((ng,)), dma((ng,)), dma((ng,)), dma((ng,)), dma((ng,)), dma((ng,)), dma((8,)),
        ],
        compiler_params=pltpu.CompilerParams(
            collective_id=0, has_side_effects=True, vmem_limit_bytes=48 * 2**20
        ),
    )(activations, cotangent, carried_error, owner_error)
    return pl.pallas_call(
        expand_kernel,
        grid=(B,),
        in_specs=[pl.BlockSpec((2, 1, 3, 4, 16, 8, 128), lambda b: (0, b, 0, 0, 0, 0, 0))],
        out_specs=pl.BlockSpec((ROWS, D), lambda b: (b, 0)),
        out_shape=jax.ShapeDtypeStruct((D, D), f32),
        compiler_params=pltpu.CompilerParams(vmem_limit_bytes=16 * 2**20),
    )(gathered)


def solution(mesh):
    return jax.shard_map(
        on_device,
        mesh=mesh,
        in_specs=(
            P(("grp", "dp"), None),
            P(("grp", "dp"), None),
            P(("grp", "dp"), None, None),
            P(("grp", "dp"), None),
        ),
        out_specs=P(),
        check_vma=False,
    )
```

```python
import jax
import jax.numpy as jnp
from jax import lax
from jax.experimental import pallas as pl
from jax.experimental.pallas import tpu as pltpu
from jax.sharding import PartitionSpec as P

D = 1280
BLOCK = 128
TOK = 2048
MESH = pl.DeviceIdType.MESH
B = 5
ROWS = D // B
TILES = ROWS // 8
HALF = 5
CHUNKS = 5
WIDE = D // CHUNKS
KS = (3, 3, 2)
OFFS = (0, 12, 24)
KOFF = (0, 3, 6)
ORDER = (("z", "y", "x"), ("y", "x", "z"), ("x", "z", "y"))
PLANE = [(i, j) for i in (2, 1, 3, 0) for j in (2, 1, 3, 0) if i or j]
GROUPS = ((0, 2), (2, 2), (4, 1))


def quantized(x):
    largest = jnp.max(jnp.abs(x), axis=-1, keepdims=True)
    scale = ((largest + 1e-06) / 127.0).astype(jnp.bfloat16).astype(jnp.float32)
    level = (x * (1.0 / scale)).astype(jnp.bfloat16).astype(jnp.float32)
    return level * scale


def places():
    g, d = lax.axis_index("grp"), lax.axis_index("dp")
    return {
        "core": lax.rem(g, 2),
        "z": 2 * (d // 16) + g // 2,
        "y": lax.rem(d // 4, 4),
        "x": lax.rem(d, 4),
    }


def device_at(place):
    z = place["z"]
    return (2 * lax.rem(z, 2) + place["core"], 16 * (z // 2) + 4 * place["y"] + place["x"])


def along(place, axis, step):
    return {**place, axis: lax.rem(place[axis] + step, 4)}


def across(place, c, steps):
    return along(along(place, ORDER[c][1], steps[0]), ORDER[c][2], steps[1])


def reduce_kernel(
    a_hbm, c_hbm, e_hbm, oe_hbm, g_ref,
    a_v, c_v, e_v, oe_v, at_0, at_1, pad_v, q, rx0, s, r1, t, r2,
    a_sem, c_sem, e_sem, oe_sem, d2d_recv, p1_recv, p2_recv, g2_recv, g1_recv, gd_recv, sent,
):
    me = places()
    core = me["core"]
    partner = {**me, "core": 1 - core}
    slot = [4 * me[ORDER[c][1]] + me[ORDER[c][2]] for c in range(3)]

    def load_a(b):
        return pltpu.make_async_copy(a_hbm.at[:, pl.ds(b * ROWS, ROWS)], a_v.at[b], a_sem.at[b])

    def load_e(b):
        return pltpu.make_async_copy(e_hbm.at[0, pl.ds(b * ROWS, ROWS), :], e_v.at[b], e_sem.at[b])

    def columns(n):
        return pl.ds(n * WIDE, WIDE)

    def load_c(n):
        return pltpu.make_async_copy(c_hbm.at[:, columns(n)], c_v.at[:, columns(n)], c_sem.at[n])

    load_a(0).start()
    load_c(0).start()
    load_oe = pltpu.make_async_copy(oe_hbm, oe_v, oe_sem)
    load_oe.start()

    peers = [partner] + [along(me, axis, step) for axis in "xyz" for step in (1, 2, 3)]
    peers += [across(me, c, steps) for c in range(3) for steps in PLANE if steps[0] and steps[1]]
    barrier = pltpu.get_barrier_semaphore()
    for peer in peers:
        pl.semaphore_signal(barrier, inc=1, device_id=device_at(peer), device_id_type=MESH)

    load_c(1).start()
    load_c(2).start()
    load_e(0).start()

    def push(src, dst, peer, send, recv):
        pltpu.make_async_remote_copy(
            src_ref=src, dst_ref=dst, send_sem=send, recv_sem=recv,
            device_id=device_at(peer), device_id_type=MESH,
        ).start()

    def landed(ref, sem):
        pltpu.make_async_copy(ref, ref, sem).wait()

    index = lax.axis_index("grp") * 32 + lax.axis_index("dp")
    first_tile = (10 * index) // 8
    shift = 10 * index - 8 * first_tile
    load_oe.wait()
    row = lax.broadcasted_iota(jnp.int32, (16, D), 0)
    padded = jnp.zeros((16, D), jnp.float32)
    for r in range(10):
        padded = jnp.where(row == shift + r, oe_v[r : r + 1, :], padded)
    for h in range(2):
        for j in range(HALF):
            for w in range(2):
                col = (h * HALF + j) * 128
                pad_v[h, w, j] = padded[8 * w : 8 * w + 8, col : col + 128]

    def add_owner_error(b, half):
        for w in range(2):
            tile = first_tile + w
            i = lax.rem(tile, TILES)
            extra = jnp.where(tile // TILES == b, pad_v[half, w], 0.0)
            q[b, half, i] = (q[b, half, i].astype(jnp.float32) + extra).astype(jnp.bfloat16)

    def multiply(b, n, at_v):
        x = jnp.dot(at_v[...], c_v[:, columns(n)], preferred_element_type=jnp.float32)
        x = x + e_v[b, :, columns(n)]
        for u in range(2):
            at = 2 * n + u
            own = quantized(x[:, u * 128 : (u + 1) * 128])
            q[b, at // HALF, :, at % HALF] = own.astype(jnp.bfloat16).reshape(TILES, 8, 128)

    def to_partner(b):
        for half in range(2):
            add_owner_error(b, half)
        push(q.at[b, 1 - core], rx0.at[b], partner, sent.at[0], d2d_recv.at[b])

    def chip_sum(b):
        landed(rx0.at[b], d2d_recv.at[b])
        s[b] = (q[b, core].astype(jnp.float32) + rx0[b].astype(jnp.float32)).astype(jnp.bfloat16)
        for step in (2, 1, 3):
            for c in range(3):
                peer = along(me, ORDER[c][0], step)
                at = OFFS[c] + peer[ORDER[c][0]] * KS[c]
                push(
                    s.at[b, pl.ds(at, KS[c])], r1.at[b, step - 1, pl.ds(KOFF[c], KS[c])],
                    peer, sent.at[1], p1_recv.at[b],
                )

    def first_sum(b):
        landed(r1.at[b], p1_recv.at[b])
        for c in range(3):
            total = s[b, pl.ds(OFFS[c] + me[ORDER[c][0]] * KS[c], KS[c])].astype(jnp.float32)
            for step in range(3):
                total = total + r1[b, step, KOFF[c] : KOFF[c] + KS[c]].astype(jnp.float32)
            t[b, c, 0 : 5 * KS[c]] = total.astype(jnp.bfloat16).reshape(5 * KS[c], 8, 128)

    def plane_send(i):
        b, nb = GROUPS[i]
        for k, steps in enumerate(PLANE):
            for c in range(3):
                peer = across(me, c, steps)
                at = 4 * peer[ORDER[c][1]] + peer[ORDER[c][2]]
                push(
                    t.at[pl.ds(b, nb), c, at], r2.at[pl.ds(b, nb), c, k],
                    peer, sent.at[2], p2_recv.at[i],
                )

    def own_update(i):
        b, nb = GROUPS[i]
        landed(r2.at[pl.ds(b, nb)], p2_recv.at[i])
        for c in range(3):
            total = t[b : b + nb, c, slot[c]].astype(jnp.float32)
            for k in range(15):
                total = total + r2[b : b + nb, c, k].astype(jnp.float32)
            g_ref[core, b : b + nb, c, me[ORDER[c][0]], slot[c]] = quantized(total).astype(jnp.bfloat16)
        for steps in PLANE:
            for c in range(3):
                ref = g_ref.at[core, pl.ds(b, nb), c, me[ORDER[c][0]], slot[c]]
                push(ref, ref, across(me, c, steps), sent.at[3], g2_recv.at[i])

    def piece(i, c, place):
        b, nb = GROUPS[i]
        return g_ref.at[core, pl.ds(b, nb), c, place, pl.ds(0, 5 * KS[c])]

    def forward(i, step):
        for c in range(3):
            ref = piece(i, c, lax.rem(me[ORDER[c][0]] + 4 - step, 4))
            push(ref, ref, partner, sent.at[5], gd_recv.at[i])

    def spread(i):
        b, nb = GROUPS[i]
        landed(r2.at[pl.ds(b, nb)], g2_recv.at[i])
        for step in (2, 1, 3):
            for c in range(3):
                ref = piece(i, c, me[ORDER[c][0]])
                push(ref, ref, along(me, ORDER[c][0], step), sent.at[4], g1_recv.at[i, step - 1])
        forward(i, 0)

    def pass_on(i):
        b, nb = GROUPS[i]
        for step in (1, 3, 2):
            landed(r1.at[pl.ds(b, nb), 0], g1_recv.at[i, step - 1])
            forward(i, step)

    load_a(0).wait()
    load_c(3).start()
    load_c(4).start()
    load_a(1).start()
    at_0[...] = a_v[0].T
    for n in range(3):
        load_c(n).wait()
    load_e(0).wait()
    load_e(1).start()
    load_a(2).start()
    for n in range(3):
        multiply(0, n, at_0)
    load_c(3).wait()
    load_c(4).wait()
    load_e(2).start()
    load_a(3).start()
    for n in range(3, CHUNKS):
        multiply(0, n, at_0)
    pl.semaphore_wait(barrier, len(peers))
    to_partner(0)

    def block(b, at_v):
        load_a(b).wait()
        load_e(b).wait()

        @pl.when(b < B - 2)
        def _():
            load_e(b + 2).start()

        @pl.when(b < B - 3)
        def _():
            load_a(b + 3).start()

        at_v[...] = a_v[b].T
        for n in range(CHUNKS):
            multiply(b, n, at_v)
        to_partner(b)
        chip_sum(b - 1)

    def pair(k, carry):
        block(2 * k + 1, at_1)
        block(2 * k + 2, at_0)
        return carry

    lax.fori_loop(0, (B - 1) // 2, pair, 0)
    first_sum(0)
    first_sum(1)
    plane_send(0)
    chip_sum(B - 1)
    first_sum(2)
    first_sum(3)
    plane_send(1)
    first_sum(4)
    plane_send(2)
    own_update(0)
    own_update(1)
    own_update(2)
    spread(0)
    spread(1)
    pass_on(0)
    spread(2)
    pass_on(1)
    pass_on(2)
    for i, (b, nb) in enumerate(GROUPS):
        landed(rx0.at[pl.ds(b, nb)], gd_recv.at[i])
    landed(rx0, sent.at[0])
    landed(r1, sent.at[1])
    landed(r2, sent.at[2])
    landed(r2, sent.at[3])
    landed(r1, sent.at[4])
    landed(rx0, sent.at[5])


def expand_kernel(g_ref, out_hbm, rows_v, sem):
    copies = []
    for b in range(B):
        for h in range(2):
            for c in range(3):
                for a in range(4):
                    for k in range(KS[c]):
                        row = 8 * (OFFS[c] + a * KS[c] + k)
                        for j in range(HALF):
                            col = (h * HALF + j) * 128
                            rows_v[b, row : row + 8, col : col + 128] = g_ref[h, b, c, a, 5 * k + j].astype(jnp.float32)
        copies.append(pltpu.make_async_copy(rows_v.at[b], out_hbm.at[pl.ds(b * ROWS, ROWS)], sem.at[b]))
        copies[-1].start()
    for copy in copies:
        copy.wait()


def on_device(activations, cotangent, carried_error, owner_error):
    any_spec = pl.BlockSpec(memory_space=pltpu.HBM)
    bf16, f32, dma = jnp.bfloat16, jnp.float32, pltpu.SemaphoreType.DMA
    shape = (2, B, 3, 4, 16, 8, 128)
    ng = len(GROUPS)
    gathered = pl.pallas_call(
        reduce_kernel,
        out_shape=jax.ShapeDtypeStruct(shape, bf16),
        in_specs=[any_spec] * 4,
        out_specs=pl.BlockSpec(memory_space=pltpu.VMEM),
        scratch_shapes=[
            pltpu.VMEM((B, TOK, ROWS), bf16),
            pltpu.VMEM((TOK, D), bf16),
            pltpu.VMEM((B, ROWS, D), f32),
            pltpu.VMEM((10, D), f32),
            pltpu.VMEM((ROWS, TOK), bf16),
            pltpu.VMEM((ROWS, TOK), bf16),
            pltpu.VMEM((2, 2, HALF, 8, 128), f32),
            pltpu.VMEM((B, 2, TILES, HALF, 8, 128), bf16),
            pltpu.VMEM((B, TILES, HALF, 8, 128), bf16),
            pltpu.VMEM((B, TILES, HALF, 8, 128), bf16),
            pltpu.VMEM((B, 3, 8, HALF, 8, 128), bf16),
            pltpu.VMEM((B, 3, 16, 8, 128), bf16),
            pltpu.VMEM((B, 3, 15, 8, 128), bf16),
            dma((B,)), dma((CHUNKS,)), dma((B,)), dma, dma((B,)), dma((B,)),
            dma((ng,)), dma((ng,)), dma((ng, 3)), dma((ng,)), dma((6,)),
        ],
        compiler_params=pltpu.CompilerParams(
            collective_id=0, has_side_effects=True, vmem_limit_bytes=48 * 2**20
        ),
    )(*(pltpu.with_memory_space_constraint(v, pltpu.HBM) for v in (activations, cotangent, carried_error, owner_error)))
    return pl.pallas_call(
        expand_kernel,
        in_specs=[pl.BlockSpec(memory_space=pltpu.VMEM)],
        out_specs=any_spec,
        out_shape=jax.ShapeDtypeStruct((D, D), f32),
        scratch_shapes=[pltpu.VMEM((B, ROWS, D), f32), dma((B,))],
        compiler_params=pltpu.CompilerParams(vmem_limit_bytes=16 * 2**20),
    )(gathered)


def solution(mesh):
    return jax.shard_map(
        on_device,
        mesh=mesh,
        in_specs=(
            P(("grp", "dp"), None),
            P(("grp", "dp"), None),
            P(("grp", "dp"), None, None),
            P(("grp", "dp"), None),
        ),
        out_specs=P(),
        check_vma=False,
    )
```

```python
import jax
import jax.numpy as jnp
from jax import lax
from jax.experimental import pallas as pl
from jax.experimental.pallas import tpu as pltpu
from jax.sharding import PartitionSpec as P

D = 1280
BLOCK = 128
TOK = 2048
MESH = pl.DeviceIdType.MESH
B = 5
ROWS = D // B
TILES = ROWS // 8
HALF = 5
CHUNKS = 5
WIDE = D // CHUNKS
KS = (3, 3, 2)
OFFS = (0, 12, 24)
KOFF = (0, 3, 6)
ORDER = (("z", "y", "x"), ("y", "x", "z"), ("x", "z", "y"))
PLANE = [(i, j) for i in (2, 1, 3, 0) for j in (2, 1, 3, 0) if i or j]
GROUPS = ((0, 3), (3, 2))


def quantized(x):
    largest = jnp.max(jnp.abs(x), axis=-1, keepdims=True)
    scale = ((largest + 1e-06) / 127.0).astype(jnp.bfloat16).astype(jnp.float32)
    level = (x * (1.0 / scale)).astype(jnp.bfloat16).astype(jnp.float32)
    return level * scale


def places():
    g, d = lax.axis_index("grp"), lax.axis_index("dp")
    return {
        "core": lax.rem(g, 2),
        "z": 2 * (d // 16) + g // 2,
        "y": lax.rem(d // 4, 4),
        "x": lax.rem(d, 4),
    }


def device_at(place):
    z = place["z"]
    return (2 * lax.rem(z, 2) + place["core"], 16 * (z // 2) + 4 * place["y"] + place["x"])


def along(place, axis, step):
    return {**place, axis: lax.rem(place[axis] + step, 4)}


def across(place, c, steps):
    return along(along(place, ORDER[c][1], steps[0]), ORDER[c][2], steps[1])


def reduce_kernel(
    a_hbm, c_hbm, e_hbm, oe_hbm, g_ref,
    a_v, c_v, e_v, oe_v, at_0, at_1, pad_v, q, rx0, s, r1, t, r2,
    a_sem, c_sem, e_sem, oe_sem, d2d_recv, p1_recv, p2_recv, g2_recv, g1_recv, gd_recv, sent,
):
    me = places()
    core = me["core"]
    partner = {**me, "core": 1 - core}
    slot = [4 * me[ORDER[c][1]] + me[ORDER[c][2]] for c in range(3)]

    def load_a(b):
        return pltpu.make_async_copy(a_hbm.at[:, pl.ds(b * ROWS, ROWS)], a_v.at[b], a_sem.at[b])

    def load_e(b):
        return pltpu.make_async_copy(e_hbm.at[0, pl.ds(b * ROWS, ROWS), :], e_v.at[b], e_sem.at[b])

    def columns(n):
        return pl.ds(n * WIDE, WIDE)

    def load_c(n):
        return pltpu.make_async_copy(c_hbm.at[:, columns(n)], c_v.at[:, columns(n)], c_sem.at[n])

    load_a(0).start()
    load_c(0).start()
    load_oe = pltpu.make_async_copy(oe_hbm, oe_v, oe_sem)
    load_oe.start()

    peers = [partner] + [along(me, axis, step) for axis in "xyz" for step in (1, 2, 3)]
    barrier = pltpu.get_barrier_semaphore()
    for peer in peers:
        pl.semaphore_signal(barrier, inc=1, device_id=device_at(peer), device_id_type=MESH)

    load_c(1).start()
    load_c(2).start()
    load_e(0).start()

    def push(src, dst, peer, send, recv):
        pltpu.make_async_remote_copy(
            src_ref=src, dst_ref=dst, send_sem=send, recv_sem=recv,
            device_id=device_at(peer), device_id_type=MESH,
        ).start()

    def landed(ref, sem):
        pltpu.make_async_copy(ref, ref, sem).wait()

    index = lax.axis_index("grp") * 32 + lax.axis_index("dp")
    first_tile = (10 * index) // 8
    shift = 10 * index - 8 * first_tile
    load_oe.wait()
    row = lax.broadcasted_iota(jnp.int32, (16, D), 0)
    padded = jnp.zeros((16, D), jnp.float32)
    for r in range(10):
        padded = jnp.where(row == shift + r, oe_v[r : r + 1, :], padded)
    for h in range(2):
        for j in range(HALF):
            for w in range(2):
                col = (h * HALF + j) * 128
                pad_v[h, w, j] = padded[8 * w : 8 * w + 8, col : col + 128]

    def add_owner_error(b, half):
        for w in range(2):
            tile = first_tile + w
            i = lax.rem(tile, TILES)
            extra = jnp.where(tile // TILES == b, pad_v[half, w], 0.0)
            q[b, half, i] = (q[b, half, i].astype(jnp.float32) + extra).astype(jnp.bfloat16)

    def multiply(b, n, at_v):
        x = jnp.dot(at_v[...], c_v[:, columns(n)], preferred_element_type=jnp.float32)
        x = x + e_v[b, :, columns(n)]
        for u in range(2):
            at = 2 * n + u
            own = quantized(x[:, u * 128 : (u + 1) * 128])
            q[b, at // HALF, :, at % HALF] = own.astype(jnp.bfloat16).reshape(TILES, 8, 128)

    def to_partner(b):
        for half in range(2):
            add_owner_error(b, half)
        push(q.at[b, 1 - core], rx0.at[b], partner, sent.at[0], d2d_recv.at[b])

    def chip_sum(b):
        landed(rx0.at[b], d2d_recv.at[b])
        s[b] = (q[b, core].astype(jnp.float32) + rx0[b].astype(jnp.float32)).astype(jnp.bfloat16)
        for step in (2, 1, 3):
            for c in range(3):
                peer = along(me, ORDER[c][0], step)
                at = OFFS[c] + peer[ORDER[c][0]] * KS[c]
                push(
                    s.at[b, pl.ds(at, KS[c])], r1.at[b, step - 1, pl.ds(KOFF[c], KS[c])],
                    peer, sent.at[1], p1_recv.at[b],
                )

    def first_sum(b):
        landed(r1.at[b], p1_recv.at[b])
        for c in range(3):
            total = s[b, pl.ds(OFFS[c] + me[ORDER[c][0]] * KS[c], KS[c])].astype(jnp.float32)
            for step in range(3):
                total = total + r1[b, step, KOFF[c] : KOFF[c] + KS[c]].astype(jnp.float32)
            t[b, c, 0 : 5 * KS[c]] = total.astype(jnp.bfloat16).reshape(5 * KS[c], 8, 128)

    def plane_send(i):
        b, nb = GROUPS[i]
        for k, steps in enumerate(PLANE):
            for c in range(3):
                peer = across(me, c, steps)
                at = 4 * peer[ORDER[c][1]] + peer[ORDER[c][2]]
                push(
                    t.at[pl.ds(b, nb), c, at], r2.at[pl.ds(b, nb), c, k],
                    peer, sent.at[2], p2_recv.at[i],
                )

    def own_update(i):
        b, nb = GROUPS[i]
        landed(r2.at[pl.ds(b, nb)], p2_recv.at[i])
        for c in range(3):
            total = t[b : b + nb, c, slot[c]].astype(jnp.float32)
            for k in range(15):
                total = total + r2[b : b + nb, c, k].astype(jnp.float32)
            g_ref[core, b : b + nb, c, me[ORDER[c][0]], slot[c]] = quantized(total).astype(jnp.bfloat16)
        for steps in PLANE:
            for c in range(3):
                ref = g_ref.at[core, pl.ds(b, nb), c, me[ORDER[c][0]], slot[c]]
                push(ref, ref, across(me, c, steps), sent.at[3], g2_recv.at[i])

    def piece(i, c, place):
        b, nb = GROUPS[i]
        return g_ref.at[core, pl.ds(b, nb), c, place, pl.ds(0, 5 * KS[c])]

    def forward(i, step):
        for c in range(3):
            ref = piece(i, c, lax.rem(me[ORDER[c][0]] + 4 - step, 4))
            push(ref, ref, partner, sent.at[5], gd_recv.at[i])

    def spread(i):
        b, nb = GROUPS[i]
        landed(r2.at[pl.ds(b, nb)], g2_recv.at[i])
        for step in (2, 1, 3):
            for c in range(3):
                ref = piece(i, c, me[ORDER[c][0]])
                push(ref, ref, along(me, ORDER[c][0], step), sent.at[4], g1_recv.at[i, step - 1])
        forward(i, 0)

    def pass_on(i):
        b, nb = GROUPS[i]
        for step in (1, 3, 2):
            landed(r1.at[pl.ds(b, nb), 0], g1_recv.at[i, step - 1])
            forward(i, step)

    load_a(0).wait()
    load_c(3).start()
    load_c(4).start()
    load_a(1).start()
    at_0[...] = a_v[0].T
    for n in range(3):
        load_c(n).wait()
    load_e(0).wait()
    load_e(1).start()
    load_a(2).start()
    for n in range(3):
        multiply(0, n, at_0)
    load_c(3).wait()
    load_c(4).wait()
    load_e(2).start()
    load_a(3).start()
    for n in range(3, CHUNKS):
        multiply(0, n, at_0)

    def block(b):
        load_a(b).wait()
        load_e(b).wait()

        @pl.when(b < B - 2)
        def _():
            load_e(b + 2).start()

        @pl.when(b < B - 3)
        def _():
            load_a(b + 3).start()

        at_1[...] = a_v[b].T
        for n in range(CHUNKS):
            multiply(b, n, at_1)

    block(1)
    pl.semaphore_wait(barrier, len(peers))
    to_partner(0)
    to_partner(1)

    def step(b, carry):
        block(b)
        to_partner(b)

        @pl.when(b == 2)
        def _():
            chip_sum(0)

        chip_sum(b - 1)
        return carry

    lax.fori_loop(2, B, step, 0)
    first_sum(0)
    first_sum(1)
    chip_sum(B - 1)
    first_sum(2)
    plane_send(0)
    first_sum(3)
    first_sum(4)
    plane_send(1)
    own_update(0)
    own_update(1)
    spread(0)
    spread(1)
    pass_on(0)
    pass_on(1)
    for i, (b, nb) in enumerate(GROUPS):
        landed(rx0.at[pl.ds(b, nb)], gd_recv.at[i])
    landed(rx0, sent.at[0])
    landed(r1, sent.at[1])
    landed(r2, sent.at[2])
    landed(r2, sent.at[3])
    landed(r1, sent.at[4])
    landed(rx0, sent.at[5])


def expand_kernel(g_ref, out_hbm, rows_v, sem):
    copies = []
    for b in range(B):
        for h in range(2):
            for c in range(3):
                for a in range(4):
                    for k in range(KS[c]):
                        row = 8 * (OFFS[c] + a * KS[c] + k)
                        for j in range(HALF):
                            col = (h * HALF + j) * 128
                            rows_v[b, row : row + 8, col : col + 128] = g_ref[h, b, c, a, 5 * k + j].astype(jnp.float32)
        copies.append(pltpu.make_async_copy(rows_v.at[b], out_hbm.at[pl.ds(b * ROWS, ROWS)], sem.at[b]))
        copies[-1].start()
    for copy in copies:
        copy.wait()


def on_device(activations, cotangent, carried_error, owner_error):
    any_spec = pl.BlockSpec(memory_space=pltpu.HBM)
    bf16, f32, dma = jnp.bfloat16, jnp.float32, pltpu.SemaphoreType.DMA
    shape = (2, B, 3, 4, 16, 8, 128)
    ng = len(GROUPS)
    gathered = pl.pallas_call(
        reduce_kernel,
        out_shape=jax.ShapeDtypeStruct(shape, bf16),
        in_specs=[any_spec] * 4,
        out_specs=pl.BlockSpec(memory_space=pltpu.VMEM),
        scratch_shapes=[
            pltpu.VMEM((B, TOK, ROWS), bf16),
            pltpu.VMEM((TOK, D), bf16),
            pltpu.VMEM((B, ROWS, D), f32),
            pltpu.VMEM((10, D), f32),
            pltpu.VMEM((ROWS, TOK), bf16),
            pltpu.VMEM((ROWS, TOK), bf16),
            pltpu.VMEM((2, 2, HALF, 8, 128), f32),
            pltpu.VMEM((B, 2, TILES, HALF, 8, 128), bf16),
            pltpu.VMEM((B, TILES, HALF, 8, 128), bf16),
            pltpu.VMEM((B, TILES, HALF, 8, 128), bf16),
            pltpu.VMEM((B, 3, 8, HALF, 8, 128), bf16),
            pltpu.VMEM((B, 3, 16, 8, 128), bf16),
            pltpu.VMEM((B, 3, 15, 8, 128), bf16),
            dma((B,)), dma((CHUNKS,)), dma((B,)), dma, dma((B,)), dma((B,)),
            dma((ng,)), dma((ng,)), dma((ng, 3)), dma((ng,)), dma((6,)),
        ],
        compiler_params=pltpu.CompilerParams(
            collective_id=0, has_side_effects=True, vmem_limit_bytes=48 * 2**20
        ),
    )(*(pltpu.with_memory_space_constraint(v, pltpu.HBM) for v in (activations, cotangent, carried_error, owner_error)))
    return pl.pallas_call(
        expand_kernel,
        in_specs=[pl.BlockSpec(memory_space=pltpu.VMEM)],
        out_specs=any_spec,
        out_shape=jax.ShapeDtypeStruct((D, D), f32),
        scratch_shapes=[pltpu.VMEM((B, ROWS, D), f32), dma((B,))],
        compiler_params=pltpu.CompilerParams(vmem_limit_bytes=16 * 2**20),
    )(gathered)


def solution(mesh):
    return jax.shard_map(
        on_device,
        mesh=mesh,
        in_specs=(
            P(("grp", "dp"), None),
            P(("grp", "dp"), None),
            P(("grp", "dp"), None, None),
            P(("grp", "dp"), None),
        ),
        out_specs=P(),
        check_vma=False,
    )
```

```python
import jax
import jax.numpy as jnp
from jax import lax
from jax.experimental import pallas as pl
from jax.experimental.pallas import tpu as pltpu
from jax.sharding import PartitionSpec as P

D = 1280
BLOCK = 128
TOK = 2048
MESH = pl.DeviceIdType.MESH
B = 5
ROWS = D // B
TILES = ROWS // 8
HALF = 5
CHUNKS = 5
WIDE = D // CHUNKS
KS = (3, 3, 2)
OFFS = (0, 12, 24)
KOFF = (0, 3, 6)
ORDER = (("z", "y", "x"), ("y", "x", "z"), ("x", "z", "y"))
PLANE = [(i, j) for i in range(4) for j in range(4) if i or j]
PLANE.sort(key=lambda at: -(at[0] % 2 + at[1] % 2 + 2 * (at[0] == 2) + 2 * (at[1] == 2)))
GROUPS = ((0, 3), (3, 2))


def quantized(x):
    largest = jnp.max(jnp.abs(x), axis=-1, keepdims=True)
    scale = ((largest + 1e-06) / 127.0).astype(jnp.bfloat16).astype(jnp.float32)
    level = (x * (1.0 / scale)).astype(jnp.bfloat16).astype(jnp.float32)
    return level * scale


def places():
    g, d = lax.axis_index("grp"), lax.axis_index("dp")
    return {
        "core": lax.rem(g, 2),
        "z": 2 * (d // 16) + g // 2,
        "y": lax.rem(d // 4, 4),
        "x": lax.rem(d, 4),
    }


def device_at(place):
    z = place["z"]
    return (2 * lax.rem(z, 2) + place["core"], 16 * (z // 2) + 4 * place["y"] + place["x"])


def along(place, axis, step):
    return {**place, axis: lax.rem(place[axis] + step, 4)}


def across(place, c, steps):
    return along(along(place, ORDER[c][1], steps[0]), ORDER[c][2], steps[1])


def reduce_kernel(
    a_hbm, c_hbm, e_hbm, oe_hbm, g_ref,
    a_v, c_v, e_v, oe_v, at_0, at_1, pad_v, q, rx0, s, r1, t, r2,
    a_sem, c_sem, e_sem, oe_sem, d2d_recv, p1_recv, p2_recv, g2_recv, g1_recv, gd_recv, sent,
):
    me = places()
    core = me["core"]
    partner = {**me, "core": 1 - core}
    slot = [4 * me[ORDER[c][1]] + me[ORDER[c][2]] for c in range(3)]

    def load_a(b):
        return pltpu.make_async_copy(a_hbm.at[:, pl.ds(b * ROWS, ROWS)], a_v.at[b], a_sem.at[b])

    def load_e(b):
        return pltpu.make_async_copy(e_hbm.at[0, pl.ds(b * ROWS, ROWS), :], e_v.at[b], e_sem.at[b])

    def columns(n):
        return pl.ds(n * WIDE, WIDE)

    def load_c(n):
        return pltpu.make_async_copy(c_hbm.at[:, columns(n)], c_v.at[:, columns(n)], c_sem.at[n])

    load_a(0).start()
    load_c(0).start()
    load_oe = pltpu.make_async_copy(oe_hbm, oe_v, oe_sem)
    load_oe.start()

    peers = [partner] + [along(me, axis, step) for axis in "xyz" for step in (1, 2, 3)]
    barrier = pltpu.get_barrier_semaphore()
    for peer in peers:
        pl.semaphore_signal(barrier, inc=1, device_id=device_at(peer), device_id_type=MESH)

    load_c(1).start()
    load_c(2).start()
    load_e(0).start()

    def push(src, dst, peer, send, recv):
        pltpu.make_async_remote_copy(
            src_ref=src, dst_ref=dst, send_sem=send, recv_sem=recv,
            device_id=device_at(peer), device_id_type=MESH,
        ).start()

    def landed(ref, sem):
        pltpu.make_async_copy(ref, ref, sem).wait()

    index = lax.axis_index("grp") * 32 + lax.axis_index("dp")
    first_tile = (10 * index) // 8
    shift = 10 * index - 8 * first_tile
    load_oe.wait()
    row = lax.broadcasted_iota(jnp.int32, (16, D), 0)
    padded = jnp.zeros((16, D), jnp.float32)
    for r in range(10):
        padded = jnp.where(row == shift + r, oe_v[r : r + 1, :], padded)
    for h in range(2):
        for j in range(HALF):
            for w in range(2):
                col = (h * HALF + j) * 128
                pad_v[h, w, j] = padded[8 * w : 8 * w + 8, col : col + 128]

    def add_owner_error(b, half):
        for w in range(2):
            tile = first_tile + w
            i = lax.rem(tile, TILES)
            extra = jnp.where(tile // TILES == b, pad_v[half, w], 0.0)
            q[b, half, i] = (q[b, half, i].astype(jnp.float32) + extra).astype(jnp.bfloat16)

    def multiply(b, n, at_v):
        x = jnp.dot(at_v[...], c_v[:, columns(n)], preferred_element_type=jnp.float32)
        x = x + e_v[b, :, columns(n)]
        for u in range(2):
            at = 2 * n + u
            own = quantized(x[:, u * 128 : (u + 1) * 128])
            q[b, at // HALF, :, at % HALF] = own.astype(jnp.bfloat16).reshape(TILES, 8, 128)

    def to_partner(b):
        for half in range(2):
            add_owner_error(b, half)
        push(q.at[b, 1 - core], rx0.at[b], partner, sent.at[0], d2d_recv.at[b])

    def chip_sum(b):
        landed(rx0.at[b], d2d_recv.at[b])
        s[b] = (q[b, core].astype(jnp.float32) + rx0[b].astype(jnp.float32)).astype(jnp.bfloat16)
        for step in (2, 1, 3):
            for c in range(3):
                peer = along(me, ORDER[c][0], step)
                at = OFFS[c] + peer[ORDER[c][0]] * KS[c]
                push(
                    s.at[b, pl.ds(at, KS[c])], r1.at[b, step - 1, pl.ds(KOFF[c], KS[c])],
                    peer, sent.at[1], p1_recv.at[b],
                )

    def first_sum(b):
        landed(r1.at[b], p1_recv.at[b])
        for c in range(3):
            total = s[b, pl.ds(OFFS[c] + me[ORDER[c][0]] * KS[c], KS[c])].astype(jnp.float32)
            for step in range(3):
                total = total + r1[b, step, KOFF[c] : KOFF[c] + KS[c]].astype(jnp.float32)
            t[b, c, 0 : 5 * KS[c]] = total.astype(jnp.bfloat16).reshape(5 * KS[c], 8, 128)

    def plane_send(i):
        b, nb = GROUPS[i]
        for k, steps in enumerate(PLANE):
            for c in range(3):
                peer = across(me, c, steps)
                at = 4 * peer[ORDER[c][1]] + peer[ORDER[c][2]]
                push(
                    t.at[pl.ds(b, nb), c, at], r2.at[pl.ds(b, nb), c, k],
                    peer, sent.at[2], p2_recv.at[i],
                )

    def own_update(i):
        b, nb = GROUPS[i]
        landed(r2.at[pl.ds(b, nb)], p2_recv.at[i])
        for c in range(3):
            total = t[b : b + nb, c, slot[c]].astype(jnp.float32)
            for k in range(15):
                total = total + r2[b : b + nb, c, k].astype(jnp.float32)
            g_ref[core, b : b + nb, c, me[ORDER[c][0]], slot[c]] = quantized(total).astype(jnp.bfloat16)
        for steps in PLANE:
            for c in range(3):
                ref = g_ref.at[core, pl.ds(b, nb), c, me[ORDER[c][0]], slot[c]]
                push(ref, ref, across(me, c, steps), sent.at[3], g2_recv.at[i])

    def piece(i, c, place):
        b, nb = GROUPS[i]
        return g_ref.at[core, pl.ds(b, nb), c, place, pl.ds(0, 5 * KS[c])]

    def forward(i, step):
        for c in range(3):
            ref = piece(i, c, lax.rem(me[ORDER[c][0]] + 4 - step, 4))
            push(ref, ref, partner, sent.at[5], gd_recv.at[i])

    def spread(i):
        b, nb = GROUPS[i]
        landed(r2.at[pl.ds(b, nb)], g2_recv.at[i])
        for step in (2, 1, 3):
            for c in range(3):
                ref = piece(i, c, me[ORDER[c][0]])
                push(ref, ref, along(me, ORDER[c][0], step), sent.at[4], g1_recv.at[i, step - 1])
        forward(i, 0)

    def pass_on(i):
        b, nb = GROUPS[i]
        for step in (1, 3, 2):
            landed(r1.at[pl.ds(b, nb), 0], g1_recv.at[i, step - 1])
            forward(i, step)

    load_a(0).wait()
    load_c(3).start()
    load_c(4).start()
    load_a(1).start()
    at_0[...] = a_v[0].T
    for n in range(3):
        load_c(n).wait()
    load_e(0).wait()
    load_e(1).start()
    load_a(2).start()
    for n in range(3):
        multiply(0, n, at_0)
    load_c(3).wait()
    load_c(4).wait()
    load_e(2).start()
    load_a(3).start()
    for n in range(3, CHUNKS):
        multiply(0, n, at_0)

    def block(b):
        load_a(b).wait()
        load_e(b).wait()

        @pl.when(b < B - 2)
        def _():
            load_e(b + 2).start()

        @pl.when(b < B - 3)
        def _():
            load_a(b + 3).start()

        at_1[...] = a_v[b].T
        for n in range(CHUNKS):
            multiply(b, n, at_1)

    block(1)
    pl.semaphore_wait(barrier, len(peers))
    to_partner(0)
    to_partner(1)

    def step(b, carry):
        block(b)
        to_partner(b)

        @pl.when(b == 2)
        def _():
            chip_sum(0)

        chip_sum(b - 1)
        return carry

    lax.fori_loop(2, B, step, 0)
    first_sum(0)
    first_sum(1)
    chip_sum(B - 1)
    first_sum(2)
    plane_send(0)
    first_sum(3)
    first_sum(4)
    plane_send(1)
    own_update(0)
    own_update(1)
    spread(0)
    spread(1)
    pass_on(0)
    pass_on(1)
    for i, (b, nb) in enumerate(GROUPS):
        landed(rx0.at[pl.ds(b, nb)], gd_recv.at[i])
    landed(rx0, sent.at[0])
    landed(r1, sent.at[1])
    landed(r2, sent.at[2])
    landed(r2, sent.at[3])
    landed(r1, sent.at[4])
    landed(rx0, sent.at[5])


def expand_kernel(g_ref, out_hbm, rows_v, sem):
    copies = []
    for b in range(B):
        for h in range(2):
            for c in range(3):
                for a in range(4):
                    for k in range(KS[c]):
                        row = 8 * (OFFS[c] + a * KS[c] + k)
                        for j in range(HALF):
                            col = (h * HALF + j) * 128
                            rows_v[b, row : row + 8, col : col + 128] = g_ref[h, b, c, a, 5 * k + j].astype(jnp.float32)
        copies.append(pltpu.make_async_copy(rows_v.at[b], out_hbm.at[pl.ds(b * ROWS, ROWS)], sem.at[b]))
        copies[-1].start()
    for copy in copies:
        copy.wait()


def on_device(activations, cotangent, carried_error, owner_error):
    any_spec = pl.BlockSpec(memory_space=pltpu.HBM)
    bf16, f32, dma = jnp.bfloat16, jnp.float32, pltpu.SemaphoreType.DMA
    shape = (2, B, 3, 4, 16, 8, 128)
    ng = len(GROUPS)
    gathered = pl.pallas_call(
        reduce_kernel,
        out_shape=jax.ShapeDtypeStruct(shape, bf16),
        in_specs=[any_spec] * 4,
        out_specs=pl.BlockSpec(memory_space=pltpu.VMEM),
        scratch_shapes=[
            pltpu.VMEM((B, TOK, ROWS), bf16),
            pltpu.VMEM((TOK, D), bf16),
            pltpu.VMEM((B, ROWS, D), f32),
            pltpu.VMEM((10, D), f32),
            pltpu.VMEM((ROWS, TOK), bf16),
            pltpu.VMEM((ROWS, TOK), bf16),
            pltpu.VMEM((2, 2, HALF, 8, 128), f32),
            pltpu.VMEM((B, 2, TILES, HALF, 8, 128), bf16),
            pltpu.VMEM((B, TILES, HALF, 8, 128), bf16),
            pltpu.VMEM((B, TILES, HALF, 8, 128), bf16),
            pltpu.VMEM((B, 3, 8, HALF, 8, 128), bf16),
            pltpu.VMEM((B, 3, 16, 8, 128), bf16),
            pltpu.VMEM((B, 3, 15, 8, 128), bf16),
            dma((B,)), dma((CHUNKS,)), dma((B,)), dma, dma((B,)), dma((B,)),
            dma((ng,)), dma((ng,)), dma((ng, 3)), dma((ng,)), dma((6,)),
        ],
        compiler_params=pltpu.CompilerParams(
            collective_id=0, has_side_effects=True, vmem_limit_bytes=48 * 2**20
        ),
    )(*(pltpu.with_memory_space_constraint(v, pltpu.HBM) for v in (activations, cotangent, carried_error, owner_error)))
    return pl.pallas_call(
        expand_kernel,
        in_specs=[pl.BlockSpec(memory_space=pltpu.VMEM)],
        out_specs=any_spec,
        out_shape=jax.ShapeDtypeStruct((D, D), f32),
        scratch_shapes=[pltpu.VMEM((B, ROWS, D), f32), dma((B,))],
        compiler_params=pltpu.CompilerParams(vmem_limit_bytes=16 * 2**20),
    )(gathered)


def solution(mesh):
    return jax.shard_map(
        on_device,
        mesh=mesh,
        in_specs=(
            P(("grp", "dp"), None),
            P(("grp", "dp"), None),
            P(("grp", "dp"), None, None),
            P(("grp", "dp"), None),
        ),
        out_specs=P(),
        check_vma=False,
    )
```
